32 devices in a mesh: dp: 4 (over y, x), fsdp: 8 (over z, core).
Axes of the slice: x: 2, y: 2, z: 4, core: 2. Of those that a mesh axis runs over, the one named last changes fastest.
Arguments:
- tokens: bfloat16 [512, 3072], P('dp'), may hold values from -6 to 6
- cotangent: bfloat16 [512, 3072], P('dp'), may hold values from -6 to 6
- routes: int32 [512, 2], P('dp'), may hold values from 0 to 3, all different within a row; in each aligned block of 128 rows (0 to 127, 128 to 255, ...) at most 64 rows name the same one
- router_weight: float32 [512, 2], P('dp'), may hold values from 0.25 to 1
- w_gate: bfloat16 [4, 3072, 8192], P('dp', None, 'fsdp'), may hold values from -0.109375 to 0.109375
- w_up: bfloat16 [4, 3072, 8192], P('dp', None, 'fsdp'), may hold values from -0.109375 to 0.109375
- w_down: bfloat16 [4, 8192, 3072], P('dp', 'fsdp'), may hold values from -0.0625 to 0.0625
Outputs:
- output: bfloat16 [512, 3072], P('dp')
- input_grad: bfloat16 [512, 3072], P('dp')
- grad_gate: bfloat16 [4, 3072, 8192], P('dp', None, 'fsdp')
- grad_up: bfloat16 [4, 3072, 8192], P('dp', None, 'fsdp')
- grad_down: bfloat16 [4, 8192, 3072], P('dp', 'fsdp')
The draws below stay inside these ranges and needn't reach their ends.
Inputs may be any that keep to these rules, and one draw needn't show every extreme that they name: `routes`: the two experts of a token differ. In the 128 rows of one batch no expert is named by more than 64 rows, a bound that some block reaches in some batches.
All inputs are finite; a program needn't handle non-finite values.
Results may differ from the reference program's by a relative error of at most 0.025.
Values may be sent and summed in bfloat16 or wider, within the bound.
No kernel may reach another device: no remote copies, remote signals or barrier semaphores. Data moves between devices by JAX's collectives and lax.ppermute only.
A program may use at most 128 MiB of HBM per device.

```python
import math
import jax
import jax.numpy as jnp
import numpy as np
from jax import lax

D = 3072
F = 8192
TOK_DEV = 128
EXPERTS = 4
CAP = 64
TOKENS = 512
N_DP = 4
N_FSDP = 8


def levels(rng, shape, shards, low, top_value):
    level = 1.0
    for dim, parts in shards:
        heights = jax.random.uniform(jax.random.fold_in(jax.random.fold_in(rng, 6), dim), (parts,), jnp.float32, low / len(shards), top_value / len(shards))
        level = level * jnp.repeat(jnp.exp(heights), shape[dim] // parts).reshape((-1,) + (1,) * (len(shape) - 1 - dim))
    return level


def assign_block(stream_key, own, number, rows, count, top, limit, lean):
    sequence = jax.random.permutation(stream_key, count)
    crowded, common = portions_of(count, rows * top, limit, lean, True), portions_of(count, rows * top, limit, lean, False)
    places = jnp.arange(count)

    def named(lengths, offset_by):
        used = int((lengths > 0).sum())
        fixed = max(1, used // 4)
        passed = fixed + (places - fixed + offset_by * (used - fixed)) % max(1, count - fixed)
        return jnp.zeros((count,), jnp.int32).at[sequence[jnp.where(places < fixed, places, passed)]].set(jnp.asarray(lengths, jnp.int32))

    lengths = jnp.where(number % 4 == 0, named(crowded, number // 4), named(common, number - number // 4 - 1))
    mixed = jax.random.permutation(jax.random.fold_in(own, 3), count)
    source_of, sink = mixed[0:count // 2 * 2:2], mixed[1:count // 2 * 2:2]
    room = jnp.minimum(lengths[source_of] - 1, limit - lengths[sink]) // 2
    room = jnp.where((source_of == sequence[0]) | (sink == sequence[0]) | (lengths[sink] == 0), 0, jnp.maximum(room, 0))
    passed = jax.random.randint(jax.random.fold_in(own, 4), (count // 2,), 0, 1 << 20) % (room + 1)
    lengths = lengths.at[source_of].add(-passed).at[sink].add(passed)
    labels = jnp.searchsorted(jnp.cumsum(lengths), jnp.arange(rows * top), side="right").astype(jnp.int32)
    grid = labels.reshape(top, rows).T
    grid = grid[jax.random.permutation(jax.random.fold_in(own, 1), rows)]
    offset_by = jax.random.randint(jax.random.fold_in(own, 2), (rows, 1), 0, top)
    return jnp.take_along_axis(grid, (jnp.arange(top)[None, :] + offset_by) % top, axis=1)


def portions_of(number_of, total, bound, skew, full):
    portions = [(1 << 20) // math.isqrt(grade ** skew) + 1 for grade in range(1, number_of + 1)]
    largest = bound if full else min(bound, max(-(-total // number_of), total * portions[0] // sum(portions)))
    least = 1 if total - largest >= number_of - 1 else 0
    given, surplus = [largest] + [least] * (number_of - 1), total - largest - least * (number_of - 1)
    while surplus > 0:
        candidates = [i for i in range(1, number_of) if given[i] < largest] or [i for i in range(1, number_of) if given[i] < bound]
        whole, budget = sum([portions[i] for i in candidates]), surplus
        for i in candidates:
            extra = min(bound - given[i], max(1, budget * portions[i] // whole), surplus)
            given[i] = given[i] + extra
            surplus = surplus - extra
    return np.array(given)


def bell_draw(key, extent, width, bound, split=(), kind=jnp.bfloat16):
    gain = levels(key, extent, split, -0.22, 0.18) if split else 1.0
    entries = jax.random.normal(key, extent, jnp.float32) * width * gain
    return jnp.minimum(jnp.maximum(entries, -bound), bound).astype(kind)


def setup_inputs(seed: int = 0) -> dict:
    seeds = jax.random.split(jax.random.key(seed), 8)
    tokens = bell_draw(seeds[0], (TOKENS, D), 1.0, 6.0, ((0, 4),))
    cotangent = bell_draw(seeds[1], (TOKENS, D), 1.0, 6.0, ((0, 4),))
    routes_keys = jax.random.split(jax.random.fold_in(seeds[2], 1), TOKENS // TOK_DEV)
    routes_turns = jax.random.permutation(jax.random.fold_in(seeds[2], 3), TOKENS // TOK_DEV)
    routes = jax.vmap(lambda own, number: assign_block(jax.random.fold_in(seeds[2], 2), own, number, TOK_DEV, N_DP, 2, CAP, 1))(routes_keys, routes_turns).reshape((TOKENS, 2))
    router_weight = jnp.clip(0.25 + 0.75 * jax.random.uniform(seeds[3], (TOKENS, 2), jnp.float32) ** levels(seeds[3], (TOKENS, 2), ((0, 4),), -0.2, 0.2), 0.25, 1.0)
    w_gate = bell_draw(seeds[4], (EXPERTS, D, F), D ** -0.5, 0.109375, ((0, 4), (2, 8)))
    w_up = bell_draw(seeds[5], (EXPERTS, D, F), D ** -0.5, 0.109375, ((0, 4), (2, 8)))
    w_down = bell_draw(seeds[6], (EXPERTS, F, D), F ** -0.5, 0.0625, ((0, 4), (1, 8)))
    return dict(tokens=tokens, cotangent=cotangent, routes=routes, router_weight=router_weight, w_gate=w_gate, w_up=w_up, w_down=w_down)


def slot_tables(routes, router_weight):
    expert_ids = jnp.arange(N_DP, dtype=jnp.int32)
    hit_table = (routes[..., None] == expert_ids).astype(jnp.int32)
    per_token = jnp.sum(hit_table, axis=2)
    before = jnp.cumsum(per_token, axis=1) - per_token
    slot_of = jnp.sum(hit_table * before[:, :, None, :], axis=3)
    slot_ids = jnp.arange(CAP, dtype=jnp.int32)
    placed = hit_table[..., None] * (slot_of[..., None, None] == slot_ids).astype(jnp.int32)
    picked = jnp.sum(placed, axis=2).astype(jnp.float32)
    weighted = jnp.sum(placed.astype(jnp.float32) * router_weight[..., None, None], axis=2)
    return picked, weighted


def expert_pass(operands):
    slot_x, slot_dy, gate_w, up_w, down_w = operands
    gate_pre = jnp.dot(slot_x, gate_w, preferred_element_type=jnp.float32)
    up_pre = jnp.dot(slot_x, up_w, preferred_element_type=jnp.float32)
    sigma = jax.nn.sigmoid(gate_pre)
    active = gate_pre * sigma
    hidden = (active * up_pre).astype(jnp.bfloat16)
    hidden_dy = jnp.dot(slot_dy, down_w.T, preferred_element_type=jnp.float32)
    gate_dy = (hidden_dy * up_pre * sigma * (1.0 + gate_pre * (1.0 - sigma))).astype(jnp.bfloat16)
    up_dy = (hidden_dy * active).astype(jnp.bfloat16)
    grad_down = jnp.dot(hidden.T, slot_dy, preferred_element_type=jnp.float32).astype(jnp.bfloat16)
    grad_gate = jnp.dot(slot_x.T, gate_dy, preferred_element_type=jnp.float32).astype(jnp.bfloat16)
    grad_up = jnp.dot(slot_x.T, up_dy, preferred_element_type=jnp.float32).astype(jnp.bfloat16)
    block_width = F // N_FSDP

    def one_block(carry, index):
        start = (index * block_width).astype(jnp.int32)
        hidden_part = lax.dynamic_slice_in_dim(hidden, start, block_width, 1)
        gate_part = lax.dynamic_slice_in_dim(gate_dy, start, block_width, 1)
        up_part = lax.dynamic_slice_in_dim(up_dy, start, block_width, 1)
        down_rows = lax.dynamic_slice_in_dim(down_w, start, block_width, 0)
        gate_cols = lax.dynamic_slice_in_dim(gate_w, start, block_width, 1)
        up_cols = lax.dynamic_slice_in_dim(up_w, start, block_width, 1)
        out_term = jnp.dot(hidden_part, down_rows, preferred_element_type=jnp.float32).astype(jnp.bfloat16)
        out_term = lax.optimization_barrier(out_term)
        back_term = (jnp.dot(gate_part, gate_cols.T, preferred_element_type=jnp.float32)
                     + jnp.dot(up_part, up_cols.T, preferred_element_type=jnp.float32)).astype(jnp.bfloat16)
        back_term = lax.optimization_barrier(back_term)
        return (carry[0] + out_term.astype(jnp.float32), carry[1] + back_term.astype(jnp.float32)), None

    zeros = jnp.zeros((slot_x.shape[0], D), jnp.float32)
    totals, unused = lax.scan(one_block, (zeros, zeros), jnp.arange(N_FSDP, dtype=jnp.int32))
    return totals[0].astype(jnp.bfloat16), totals[1].astype(jnp.bfloat16), grad_gate, grad_up, grad_down


def reference(tokens, cotangent, routes, router_weight, w_gate, w_up, w_down):
    blocks = TOKENS // TOK_DEV
    highest = lax.Precision.HIGHEST
    inputs = tokens.reshape(blocks, TOK_DEV, D).astype(jnp.float32)
    grads_in = cotangent.reshape(blocks, TOK_DEV, D).astype(jnp.float32)
    picked, weighted = slot_tables(routes.reshape(blocks, TOK_DEV, 2), router_weight.reshape(blocks, TOK_DEV, 2))
    slot_x = jnp.einsum('btec,btd->ebcd', picked, inputs, precision=highest).astype(jnp.bfloat16)
    slot_dy = jnp.einsum('btec,btd->ebcd', weighted, grads_in, precision=highest).astype(jnp.bfloat16)
    slot_x = slot_x.reshape(N_DP, blocks * CAP, D)
    slot_dy = slot_dy.reshape(N_DP, blocks * CAP, D)
    slot_out, slot_dx, grad_gate, grad_up, grad_down = lax.map(expert_pass, (slot_x, slot_dy, w_gate, w_up, w_down))
    slot_out = slot_out.reshape(N_DP, blocks, CAP, D).astype(jnp.float32)
    slot_dx = slot_dx.reshape(N_DP, blocks, CAP, D).astype(jnp.float32)
    output = jnp.einsum('btec,ebcd->btd', weighted, slot_out, precision=highest).astype(jnp.bfloat16)
    input_grad = jnp.einsum('btec,ebcd->btd', picked, slot_dx, precision=highest).astype(jnp.bfloat16)
    return (output.reshape(TOKENS, D), input_grad.reshape(TOKENS, D), grad_gate, grad_up, grad_down)
```

```python
import functools
import jax
import jax.numpy as jnp
from jax import lax
from jax.experimental import pallas as pl
from jax.experimental.pallas import tpu as pltpu
from jax.sharding import PartitionSpec as P

F32 = jnp.float32
BF16 = jnp.bfloat16
LEAD = (((0,), (0,)), ((), ()))
TRAIL = (((1,), (1,)), ((), ()))
VMEM_BYTES = 48 * 1024 * 1024


def dot(lhs, rhs, dims=None):
    if dims is None:
        return jnp.dot(lhs, rhs, preferred_element_type=F32)
    return lax.dot_general(lhs, rhs, dims, preferred_element_type=F32)


def call(body, core, operands, in_specs, out_specs, out_shape, grid, flops, name):
    return pl.pallas_call(
        body,
        grid_spec=pltpu.PrefetchScalarGridSpec(
            num_scalar_prefetch=1, grid=grid, in_specs=in_specs, out_specs=out_specs
        ),
        out_shape=out_shape,
        compiler_params=pltpu.CompilerParams(
            dimension_semantics=("arbitrary",) * len(grid), vmem_limit_bytes=VMEM_BYTES
        ),
        cost_estimate=pl.CostEstimate(
            flops=flops, transcendentals=0, bytes_accessed=sum(v.size * 2 for v in operands)
        ),
        name=name,
    )(core, *operands)


def whole(shape):
    return pl.BlockSpec(shape, lambda *_: (0,) * len(shape))


def pick_tables(routes, weights, experts, capacity):
    tok_rows = routes.shape[1]
    lanes = (-(-experts // 8) * 8, tok_rows)
    ids = lax.broadcasted_iota(jnp.int32, lanes, 0)
    first = routes[0:1, :] == ids
    second = routes[1:2, :] == ids
    hits = jnp.where(first, 1.0, 0.0) + jnp.where(second, 1.0, 0.0)
    weight = jnp.where(first, weights[0:1, :], 0.0) + jnp.where(second, weights[1:2, :], 0.0)
    square = (tok_rows, tok_rows)
    earlier = lax.broadcasted_iota(jnp.int32, square, 0) < lax.broadcasted_iota(jnp.int32, square, 1)
    before = dot(hits.astype(BF16), jnp.where(earlier, 1.0, 0.0).astype(BF16))
    place = jnp.where(hits > 0.5, before, -1.0).astype(jnp.int32)
    slots = lax.broadcasted_iota(jnp.int32, (capacity, tok_rows), 0)
    picked = []
    weighted = []
    for expert in range(experts):
        match = place[expert : expert + 1, :] == slots
        picked.append(jnp.where(match, 1.0, 0.0))
        weighted.append(jnp.where(match, weight[expert : expert + 1, :], 0.0))
    return jnp.concatenate(picked, axis=0), jnp.concatenate(weighted, axis=0)


def gather_body(core, routes, weights, source, out, *, experts, capacity, scaled):
    picked, weighted = pick_tables(routes[...], weights[...], experts, capacity)
    rows = dot(picked.astype(BF16), source[...])
    if scaled:
        rows = rows * jnp.sum(weighted, axis=1, keepdims=True)
    out[...] = rows.astype(BF16)


def gather_rows(core, routes, weights, source, experts, capacity, scaled):
    tok_rows, features = source.shape
    half = features // 2
    rows = experts * capacity
    return call(
        functools.partial(gather_body, experts=experts, capacity=capacity, scaled=scaled),
        core,
        (routes, weights, source),
        [
            whole((2, tok_rows)),
            whole((2, tok_rows)),
            pl.BlockSpec((tok_rows, half), lambda i, c: (0, c[0])),
        ],
        whole((rows, half)),
        jax.ShapeDtypeStruct((rows, half), BF16),
        (1,),
        2 * rows * tok_rows * half,
        "gather",
    )


def merge_body(core, routes, weights, slots, out, *, experts, capacity, scaled):
    picked, weighted = pick_tables(routes[...], weights[...], experts, capacity)
    if scaled:
        high = weighted.astype(BF16)
        low = (weighted - high.astype(F32)).astype(BF16)
        total = dot(high, slots[...], LEAD) + dot(low, slots[...], LEAD)
    else:
        total = dot(picked.astype(BF16), slots[...], LEAD)
    out[...] = total.astype(BF16)


def merge_rows(core, routes, weights, slots, experts, capacity, scaled):
    tok_rows = routes.shape[1]
    rows, half = slots.shape
    return call(
        functools.partial(merge_body, experts=experts, capacity=capacity, scaled=scaled),
        core,
        (routes, weights, slots),
        [whole((2, tok_rows)), whole((2, tok_rows)), whole((rows, half))],
        whole((tok_rows, half)),
        jax.ShapeDtypeStruct((tok_rows, half), BF16),
        (1,),
        4 * rows * tok_rows * half,
        "merge",
    )


def forward_body(core, own, sib, gate_w, up_w, hidden, active, slope):
    half = own.shape[1]
    mine = pl.ds(pl.multiple_of(core[0] * half, half), half)
    other = pl.ds(pl.multiple_of((1 - core[0]) * half, half), half)
    gate = dot(own[...], gate_w[mine, :]) + dot(sib[...], gate_w[other, :])
    up = dot(own[...], up_w[mine, :]) + dot(sib[...], up_w[other, :])
    sigma = jax.nn.sigmoid(gate)
    act = gate * sigma
    hidden[...] = (act * up).astype(BF16)
    active[...] = act.astype(BF16)
    slope[...] = (up * sigma * (1.0 + gate * (1.0 - sigma))).astype(BF16)


def forward(core, own, sib, gate_w, up_w):
    rows, half = own.shape
    features, width = gate_w.shape
    step = min(256, width)
    column = pl.BlockSpec((features, step), lambda i, c: (0, i))
    result = pl.BlockSpec((rows, step), lambda i, c: (0, i))
    return call(
        forward_body,
        core,
        (own, sib, gate_w, up_w),
        [whole((rows, half)), whole((rows, half)), column, column],
        [result] * 3,
        [jax.ShapeDtypeStruct((rows, width), BF16)] * 3,
        (width // step,),
        4 * rows * features * width,
        "forward",
    )


def out_body(core, hidden, down_w, out):
    out[...] = dot(hidden[...], down_w[...]).astype(BF16)


def out_half(core, hidden, down_w, mine):
    rows, width = hidden.shape
    half = down_w.shape[1] // 2
    step = half // 3
    return call(
        out_body,
        core,
        (hidden, down_w),
        [
            whole((rows, width)),
            pl.BlockSpec((width, step), lambda i, c: (0, i + 3 * (c[0] if mine else 1 - c[0]))),
        ],
        pl.BlockSpec((rows, step), lambda i, c: (0, i)),
        jax.ShapeDtypeStruct((rows, half), BF16),
        (3,),
        2 * rows * half * width,
        "out_mine" if mine else "out_other",
    )


def hidden_body(core, own, sib, own_w, sib_w, active, slope, gate_dy, up_dy):
    hidden_dy = dot(own[...], own_w[...], TRAIL) + dot(sib[...], sib_w[...], TRAIL)
    gate_dy[...] = (hidden_dy * slope[...].astype(F32)).astype(BF16)
    up_dy[...] = (hidden_dy * active[...].astype(F32)).astype(BF16)


def hidden_grads(core, own, sib, down_w, active, slope):
    rows, half = own.shape
    width = down_w.shape[0]
    step = min(256, width)
    result = pl.BlockSpec((rows, step), lambda i, c: (0, i))
    return pl.pallas_call(
        hidden_body,
        grid_spec=pltpu.PrefetchScalarGridSpec(
            num_scalar_prefetch=1,
            grid=(width // step,),
            in_specs=[
                whole((rows, half)),
                whole((rows, half)),
                pl.BlockSpec((step, half), lambda i, c: (i, c[0])),
                pl.BlockSpec((step, half), lambda i, c: (i, 1 - c[0])),
                result,
                result,
            ],
            out_specs=[result] * 2,
        ),
        out_shape=[jax.ShapeDtypeStruct((rows, width), BF16)] * 2,
        compiler_params=pltpu.CompilerParams(
            dimension_semantics=("arbitrary",), vmem_limit_bytes=VMEM_BYTES
        ),
        name="hidden_grads",
    )(core, own, sib, down_w, down_w, active, slope)


def back_body(core, gate_dy, up_dy, gate_w, up_w, out):
    total = dot(gate_dy[...], gate_w[...], TRAIL) + dot(up_dy[...], up_w[...], TRAIL)
    out[...] = total.astype(BF16)


def back_half(core, gate_dy, up_dy, gate_w, up_w, mine):
    rows, width = gate_dy.shape
    half = gate_w.shape[0] // 2
    step = half // 3
    block = pl.BlockSpec((step, width), lambda i, c: (i + 3 * (c[0] if mine else 1 - c[0]), 0))
    return call(
        back_body,
        core,
        (gate_dy, up_dy, gate_w, up_w),
        [whole((rows, width)), whole((rows, width)), block, block],
        pl.BlockSpec((rows, step), lambda i, c: (0, i)),
        jax.ShapeDtypeStruct((rows, half), BF16),
        (3,),
        4 * rows * half * width,
        "back_mine" if mine else "back_other",
    )


def down_grad_body(core, hidden, own, sib, out):
    half = pl.program_id(0)

    @pl.when(half == core[0])
    def _():
        out[...] = dot(hidden[...], own[...], LEAD).astype(BF16)

    @pl.when(half != core[0])
    def _():
        out[...] = dot(hidden[...], sib[...], LEAD).astype(BF16)


def down_grad(core, hidden, own, sib):
    rows, width = hidden.shape
    half = own.shape[1]
    step = half // 3
    column = pl.BlockSpec((rows, step), lambda h, i, c: (0, i))
    return call(
        down_grad_body,
        core,
        (hidden, own, sib),
        [whole((rows, width)), column, column],
        pl.BlockSpec((width, step), lambda h, i, c: (0, h * 3 + i)),
        jax.ShapeDtypeStruct((width, 2 * half), BF16),
        (2, 3),
        4 * rows * half * width,
        "down_grad",
    )


def in_grads_body(core, own, sib, gate_dy, up_dy, gate_out, up_out):
    half = pl.program_id(0)

    @pl.when(half == core[0])
    def _():
        gate_out[...] = dot(own[...], gate_dy[...], LEAD).astype(BF16)
        up_out[...] = dot(own[...], up_dy[...], LEAD).astype(BF16)

    @pl.when(half != core[0])
    def _():
        gate_out[...] = dot(sib[...], gate_dy[...], LEAD).astype(BF16)
        up_out[...] = dot(sib[...], up_dy[...], LEAD).astype(BF16)


def in_grads(core, own, sib, gate_dy, up_dy):
    rows, width = gate_dy.shape
    half = own.shape[1]
    step = half // 3
    column = pl.BlockSpec((rows, step), lambda h, i, c: (0, i))
    result = pl.BlockSpec((step, width), lambda h, i, c: (h * 3 + i, 0))
    return call(
        in_grads_body,
        core,
        (own, sib, gate_dy, up_dy),
        [column, column, whole((rows, width)), whole((rows, width))],
        [result, result],
        [jax.ShapeDtypeStruct((2 * half, width), BF16)] * 2,
        (2, 3),
        8 * rows * half * width,
        "in_grads",
    )


def on_device(tokens, cotangent, routes, router_weight, w_gate, w_up, w_down):
    experts = lax.axis_size("dp")
    shards = lax.axis_size("fsdp")
    tok_rows, features = tokens.shape
    half = features // 2
    capacity = max(tok_rows * 3 // 8, tok_rows * 2 // experts, 2)
    rows = experts * capacity
    chips = shards // 2
    part = tok_rows // chips
    core = (lax.axis_index("fsdp") % 2).astype(jnp.int32).reshape(1)
    chip_groups = [list(range(k, shards, 2)) for k in range(2)]
    twins = [(i, i ^ 1) for i in range(shards)]
    routes_t = routes.T
    weights_t = router_weight.T
    gate_w = w_gate[0]
    up_w = w_up[0]
    down_w = w_down[0]

    def exchange(slots):
        moved = lax.all_to_all(
            slots.reshape(experts, capacity, half), "dp", split_axis=0, concat_axis=0, tiled=True
        )
        return moved.reshape(rows, half)

    def swap(value):
        return lax.ppermute(value, "fsdp", twins)

    def over_chips(value):
        return lax.all_to_all(
            value, "fsdp", split_axis=0, concat_axis=0, tiled=True, axis_index_groups=chip_groups
        )

    def finish(mine, other, scaled):
        slots = (mine.astype(F32) + swap(other).astype(F32)).astype(BF16)
        partial = merge_rows(
            core, routes_t, weights_t, exchange(slots), experts, capacity, scaled
        )
        parts = over_chips(partial.reshape(chips, part, half))
        total = jnp.sum(parts.astype(F32), axis=0).astype(BF16)
        spread = over_chips(jnp.broadcast_to(total[None], (chips, part, half)))
        own = spread.reshape(tok_rows, half)
        sib = swap(own)
        swapped = core[0] == 1
        return jnp.concatenate(
            [jnp.where(swapped, sib, own), jnp.where(swapped, own, sib)], axis=1
        )

    own_x = exchange(gather_rows(core, routes_t, weights_t, tokens, experts, capacity, False))
    own_dy = exchange(gather_rows(core, routes_t, weights_t, cotangent, experts, capacity, True))
    sib_x = swap(own_x)
    hidden, active, slope = forward(core, own_x, sib_x, gate_w, up_w)
    out_other = out_half(core, hidden, down_w, False)
    out_mine = out_half(core, hidden, down_w, True)
    sib_dy = swap(own_dy)
    gate_dy, up_dy = hidden_grads(core, own_dy, sib_dy, down_w, active, slope)
    back_other = back_half(core, gate_dy, up_dy, gate_w, up_w, False)
    back_mine = back_half(core, gate_dy, up_dy, gate_w, up_w, True)
    grad_down = down_grad(core, hidden, own_dy, sib_dy)
    grad_gate, grad_up = in_grads(core, own_x, sib_x, gate_dy, up_dy)
    output = finish(out_mine, out_other, True)
    input_grad = finish(back_mine, back_other, False)
    return (output, input_grad, grad_gate[None], grad_up[None], grad_down[None])


def solution(mesh):
    return jax.shard_map(
        on_device,
        mesh=mesh,
        in_specs=(
            P("dp", None),
            P("dp", None),
            P("dp", None),
            P("dp", None),
            P("dp", None, "fsdp"),
            P("dp", None, "fsdp"),
            P("dp", "fsdp", None),
        ),
        out_specs=(
            P("dp", None),
            P("dp", None),
            P("dp", None, "fsdp"),
            P("dp", None, "fsdp"),
            P("dp", "fsdp", None),
        ),
        check_vma=False,
    )
```

```python
import functools
import jax
import jax.numpy as jnp
from jax import lax
from jax.experimental import pallas as pl
from jax.experimental.pallas import tpu as pltpu
from jax.sharding import PartitionSpec as P

F32 = jnp.float32
BF16 = jnp.bfloat16
LEAD = (((0,), (0,)), ((), ()))
TRAIL = (((1,), (1,)), ((), ()))
VMEM_BYTES = 48 * 1024 * 1024


def dot(lhs, rhs, dims=None):
    if dims is None:
        return jnp.dot(lhs, rhs, preferred_element_type=F32)
    return lax.dot_general(lhs, rhs, dims, preferred_element_type=F32)


def call(body, meta, operands, in_specs, out_specs, out_shape, grid, flops, name, scratch=()):
    return pl.pallas_call(
        body,
        grid_spec=pltpu.PrefetchScalarGridSpec(
            num_scalar_prefetch=1,
            grid=grid,
            in_specs=in_specs,
            out_specs=out_specs,
            scratch_shapes=scratch,
        ),
        out_shape=out_shape,
        compiler_params=pltpu.CompilerParams(
            dimension_semantics=("arbitrary",) * len(grid), vmem_limit_bytes=VMEM_BYTES
        ),
        cost_estimate=pl.CostEstimate(
            flops=flops, transcendentals=0, bytes_accessed=sum(v.size * 2 for v in operands)
        ),
        name=name,
    )(meta, *operands)


def whole(*shape):
    return pl.BlockSpec(shape, lambda *_: (0,) * len(shape))


def array(*shape):
    return jax.ShapeDtypeStruct(shape, BF16)


def in_hbm(value):
    return pltpu.with_memory_space_constraint(value, pltpu.HBM)


def pick_tables(place_id, routes, weights, experts, capacity):
    tok_rows = routes.shape[1]
    lanes = (-(-experts // 8) * 8, tok_rows)
    ids = lax.broadcasted_iota(jnp.int32, lanes, 0) ^ place_id
    first = routes[0:1, :] == ids
    second = routes[1:2, :] == ids
    hits = jnp.where(first, 1.0, 0.0) + jnp.where(second, 1.0, 0.0)
    weight = jnp.where(first, weights[0:1, :], 0.0) + jnp.where(second, weights[1:2, :], 0.0)
    square = (tok_rows, tok_rows)
    earlier = lax.broadcasted_iota(jnp.int32, square, 0) < lax.broadcasted_iota(jnp.int32, square, 1)
    before = dot(hits.astype(BF16), jnp.where(earlier, 1.0, 0.0).astype(BF16))
    place = jnp.where(hits > 0.5, before, -1.0).astype(jnp.int32)
    slots = lax.broadcasted_iota(jnp.int32, (capacity, tok_rows), 0)
    picked = []
    weighted = []
    for expert in range(experts):
        match = place[expert : expert + 1, :] == slots
        picked.append(jnp.where(match, 1.0, 0.0))
        weighted.append(jnp.where(match, weight[expert : expert + 1, :], 0.0))
    return picked, weighted


def gather_body(meta, routes, weights, source, source_half, *outs, capacity, scaled):
    experts = len(outs)
    picked, weighted = pick_tables(meta[1], routes[...], weights[...], experts, capacity)
    for j, out in enumerate(outs):
        rows = dot(picked[j].astype(BF16), source_half[...] if j else source[...])
        if scaled:
            rows = rows * jnp.sum(weighted[j], axis=1, keepdims=True)
        out[...] = rows.astype(BF16)


def gather_rows(meta, routes, weights, source, experts, capacity, scaled):
    tok_rows, features = source.shape
    half = features // 2
    source = in_hbm(source)
    return call(
        functools.partial(gather_body, capacity=capacity, scaled=scaled),
        meta,
        (routes, weights, source, source),
        [
            whole(2, tok_rows),
            whole(2, tok_rows),
            whole(tok_rows, features),
            pl.BlockSpec((tok_rows, half), lambda i, m: (0, m[0])),
        ],
        [whole(capacity, features)] + [whole(capacity, half)] * (experts - 1),
        [array(capacity, features)] + [array(capacity, half)] * (experts - 1),
        (1,),
        2 * experts * capacity * tok_rows * half,
        "gather",
    )


def merge_body(meta, routes, weights, *refs, experts, capacity, scaled):
    slots = refs[:experts]
    send, keep, total = refs[experts:]
    picked, weighted = pick_tables(meta[1], routes[...], weights[...], experts, capacity)
    acc = None
    for j in range(experts):
        if scaled:
            high = weighted[j].astype(BF16)
            low = (weighted[j] - high.astype(F32)).astype(BF16)
            term = dot(high, slots[j][...], LEAD) + dot(low, slots[j][...], LEAD)
        else:
            term = dot(picked[j].astype(BF16), slots[j][...], LEAD)
        acc = term if acc is None else acc + term
    total[...] = acc
    count = send.shape[0]
    send[...] = total[pl.ds(pl.multiple_of((1 - meta[2]) * count, count), count), :].astype(BF16)
    keep[...] = total[pl.ds(pl.multiple_of(meta[2] * count, count), count), :].astype(BF16)


def merge_rows(meta, routes, weights, slots, scaled):
    experts = len(slots)
    tok_rows = routes.shape[1]
    capacity, half = slots[0].shape
    return call(
        functools.partial(merge_body, experts=experts, capacity=capacity, scaled=scaled),
        meta,
        (routes, weights, *slots),
        [whole(2, tok_rows), whole(2, tok_rows)] + [whole(capacity, half)] * experts,
        [whole(tok_rows // 2, half)] * 2,
        [array(tok_rows // 2, half)] * 2,
        (1,),
        4 * experts * capacity * tok_rows * half,
        "merge",
        [pltpu.VMEM((tok_rows, half), F32)],
    )


def fill_slots(meta, local, own, sib, slots):
    capacity, features = local.shape
    half = features // 2
    slots[0:capacity, :] = local[...]
    for side in range(2):

        @pl.when(meta[0] == side)
        def _():
            for j in range(len(own)):
                rows = slice((j + 1) * capacity, (j + 2) * capacity)
                mine = slice(side * half, (side + 1) * half)
                other = slice((1 - side) * half, (2 - side) * half)
                slots[rows, mine] = own[j][...]
                slots[rows, other] = sib[j][...]


def forward_body(meta, *refs, others):
    local = refs[0]
    own = refs[1 : 1 + others]
    sib = refs[1 + others : 1 + 2 * others]
    gate_w, up_w, hidden, active, slope, slots = refs[1 + 2 * others :]

    @pl.when(pl.program_id(0) == 0)
    def _():
        fill_slots(meta, local, own, sib, slots)

    gate = dot(slots[...], gate_w[...])
    up = dot(slots[...], up_w[...])
    sigma = jax.nn.sigmoid(gate)
    act = gate * sigma
    hidden[...] = (act * up).astype(BF16)
    active[...] = act.astype(BF16)
    slope[...] = (up * sigma * (1.0 + gate * (1.0 - sigma))).astype(BF16)


def forward(meta, local, own, sib, gate_w, up_w):
    capacity = local.shape[0]
    others = len(own)
    rows = capacity * (others + 1)
    features, width = gate_w.shape
    half = features // 2
    step = min(256, width)
    column = pl.BlockSpec((features, step), lambda i, m: (0, i))
    result = pl.BlockSpec((rows, step), lambda i, m: (0, i))
    return call(
        functools.partial(forward_body, others=others),
        meta,
        (local, *own, *sib, gate_w, up_w),
        [whole(capacity, features)] + [whole(capacity, half)] * (2 * others) + [column] * 2,
        [result] * 3 + [whole(rows, features)],
        [array(rows, width)] * 3 + [array(rows, features)],
        (width // step,),
        4 * rows * features * width,
        "forward",
    )


def out_other_body(meta, hidden, down_w, out):
    out[...] = dot(hidden[...], down_w[...]).astype(BF16)


def out_mine_body(meta, hidden, twin, down_w, *outs):
    total = dot(hidden[...], down_w[...]) + twin[...].astype(F32)
    capacity = outs[0].shape[0]
    for j, out in enumerate(outs):
        out[...] = total[j * capacity : (j + 1) * capacity, :].astype(BF16)


def out_half(meta, hidden, down_w, twin, experts):
    rows, width = hidden.shape
    half = down_w.shape[1] // 2
    step = half // 3
    tile = pl.BlockSpec((rows, step), lambda i, m: (0, i))
    if twin is None:
        return call(
            out_other_body,
            meta,
            (hidden, down_w),
            [whole(rows, width), pl.BlockSpec((width, step), lambda i, m: (0, i + 3 * (1 - m[0])))],
            tile,
            array(rows, half),
            (3,),
            2 * rows * half * width,
            "out_other",
        )
    return call(
        out_mine_body,
        meta,
        (hidden, twin, down_w),
        [whole(rows, width), tile, pl.BlockSpec((width, step), lambda i, m: (0, i + 3 * m[0]))],
        [pl.BlockSpec((rows // experts, step), lambda i, m: (0, i))] * experts,
        [array(rows // experts, half)] * experts,
        (3,),
        2 * rows * half * width,
        "out_mine",
    )


def hidden_body(meta, *refs, others):
    local = refs[0]
    own = refs[1 : 1 + others]
    sib = refs[1 + others : 1 + 2 * others]
    down_w, active, slope, gate_dy, up_dy, slots = refs[1 + 2 * others :]

    @pl.when(pl.program_id(0) == 0)
    def _():
        fill_slots(meta, local, own, sib, slots)

    hidden_dy = dot(slots[...], down_w[...], TRAIL)
    gate_dy[...] = (hidden_dy * slope[...].astype(F32)).astype(BF16)
    up_dy[...] = (hidden_dy * active[...].astype(F32)).astype(BF16)


def hidden_grads(meta, local, own, sib, down_w, active, slope):
    capacity, features = local.shape
    others = len(own)
    rows = capacity * (others + 1)
    half = features // 2
    width = down_w.shape[0]
    step = min(256, width)
    result = pl.BlockSpec((rows, step), lambda i, m: (0, i))
    return call(
        functools.partial(hidden_body, others=others),
        meta,
        (local, *own, *sib, down_w, active, slope),
        [whole(capacity, features)]
        + [whole(capacity, half)] * (2 * others)
        + [pl.BlockSpec((step, features), lambda i, m: (i, 0)), result, result],
        [result] * 2 + [whole(rows, features)],
        [array(rows, width)] * 2 + [array(rows, features)],
        (width // step,),
        2 * rows * features * width,
        "hidden_grads",
    )


def back_other_body(meta, gate_dy, up_dy, gate_w, up_w, out):
    total = dot(gate_dy[...], gate_w[...], TRAIL) + dot(up_dy[...], up_w[...], TRAIL)
    out[...] = total.astype(BF16)


def back_mine_body(meta, gate_dy, up_dy, twin, gate_w, up_w, *outs):
    total = dot(gate_dy[...], gate_w[...], TRAIL) + dot(up_dy[...], up_w[...], TRAIL)
    total = total + twin[...].astype(F32)
    capacity = outs[0].shape[0]
    for j, out in enumerate(outs):
        out[...] = total[j * capacity : (j + 1) * capacity, :].astype(BF16)


def back_half(meta, gate_dy, up_dy, gate_w, up_w, twin, experts):
    rows, width = gate_dy.shape
    half = gate_w.shape[0] // 2
    step = half // 3
    tile = pl.BlockSpec((rows, step), lambda i, m: (0, i))
    if twin is None:
        block = pl.BlockSpec((step, width), lambda i, m: (i + 3 * (1 - m[0]), 0))
        return call(
            back_other_body,
            meta,
            (gate_dy, up_dy, gate_w, up_w),
            [whole(rows, width), whole(rows, width), block, block],
            tile,
            array(rows, half),
            (3,),
            4 * rows * half * width,
            "back_other",
        )
    block = pl.BlockSpec((step, width), lambda i, m: (i + 3 * m[0], 0))
    return call(
        back_mine_body,
        meta,
        (gate_dy, up_dy, twin, gate_w, up_w),
        [whole(rows, width), whole(rows, width), tile, block, block],
        [pl.BlockSpec((rows // experts, step), lambda i, m: (0, i))] * experts,
        [array(rows // experts, half)] * experts,
        (3,),
        4 * rows * half * width,
        "back_mine",
    )


def down_grad_body(meta, hidden, slot_dy, out):
    out[...] = dot(hidden[...], slot_dy[...], LEAD).astype(BF16)


def down_grad(meta, hidden, slot_dy):
    rows, width = hidden.shape
    features = slot_dy.shape[1]
    step = features // 6
    return call(
        down_grad_body,
        meta,
        (hidden, slot_dy),
        [whole(rows, width), pl.BlockSpec((rows, step), lambda i, m: (0, i))],
        pl.BlockSpec((width, step), lambda i, m: (0, i)),
        array(width, features),
        (6,),
        2 * rows * features * width,
        "down_grad",
    )


def in_grads_body(meta, slot_x, gate_dy, up_dy, gate_out, up_out):
    gate_out[...] = dot(slot_x[...], gate_dy[...], LEAD).astype(BF16)
    up_out[...] = dot(slot_x[...], up_dy[...], LEAD).astype(BF16)


def in_grads(meta, slot_x, gate_dy, up_dy):
    rows, width = gate_dy.shape
    features = slot_x.shape[1]
    step = features // 6
    result = pl.BlockSpec((step, width), lambda i, m: (i, 0))
    return call(
        in_grads_body,
        meta,
        (slot_x, gate_dy, up_dy),
        [pl.BlockSpec((rows, step), lambda i, m: (0, i)), whole(rows, width), whole(rows, width)],
        [result, result],
        [array(features, width)] * 2,
        (6,),
        4 * rows * features * width,
        "in_grads",
    )


def assemble_body(meta, total, other, twin_total, twin_other, out):
    count, half = total.shape
    for keep in range(2):
        for side in range(2):

            @pl.when((meta[2] == keep) & (meta[0] == side))
            def _():
                held = slice(keep * count, (keep + 1) * count)
                rest = slice((1 - keep) * count, (2 - keep) * count)
                mine = slice(side * half, (side + 1) * half)
                theirs = slice((1 - side) * half, (2 - side) * half)
                out[held, mine] = total[...]
                out[rest, mine] = other[...]
                out[held, theirs] = twin_total[...]
                out[rest, theirs] = twin_other[...]


def assemble(meta, total, other, twin_total, twin_other):
    count, half = total.shape
    return call(
        assemble_body,
        meta,
        (total, other, twin_total, twin_other),
        [whole(count, half)] * 4,
        whole(2 * count, 2 * half),
        array(2 * count, 2 * half),
        (1,),
        0,
        "assemble",
    )


def on_device(tokens, cotangent, routes, router_weight, w_gate, w_up, w_down):
    experts = lax.axis_size("dp")
    shards = lax.axis_size("fsdp")
    tok_rows, features = tokens.shape
    capacity = max(tok_rows * 3 // 8, tok_rows * 2 // experts, 2)
    chips = shards // 2
    core = lax.axis_index("fsdp") & 1
    chip = lax.axis_index("fsdp") >> 1
    keep = (chip ^ (chip >> 1)) & 1 if chips > 2 else chip & 1
    meta = jnp.stack([core, lax.axis_index("dp"), keep]).astype(jnp.int32)
    routes_t = routes.T
    weights_t = router_weight.T
    gate_w = w_gate[0]
    up_w = w_up[0]
    down_w = w_down[0]

    def across(value, axis, offset, size):
        return lax.ppermute(value, axis, [(i, i ^ offset) for i in range(size)])

    def swap(value):
        return across(value, "fsdp", 1, shards)

    def hop(value, offset):
        return across(value, "fsdp", 2 * offset, shards)

    def exchange(blocks):
        return [across(block, "dp", j + 1, experts) for j, block in enumerate(blocks)]

    def reduce_tokens(blocks, scaled):
        slots = [blocks[0]] + exchange(blocks[1:])
        send, total = merge_rows(meta, routes_t, weights_t, slots, scaled)
        add = lambda a, b: (a.astype(F32) + b.astype(F32)).astype(BF16)
        total = add(total, hop(send, 1))
        offset = 2
        while offset < chips:
            total = add(total, hop(total, 3 if offset == 2 else offset))
            offset *= 2
        other = hop(total, 1)
        return assemble(meta, total, other, swap(total), swap(other))

    local_x, *send_x = gather_rows(meta, routes_t, weights_t, tokens, experts, capacity, False)
    own_x = exchange(send_x)
    local_dy, *send_dy = gather_rows(meta, routes_t, weights_t, cotangent, experts, capacity, True)
    own_dy = exchange(send_dy)
    sib_x = [swap(block) for block in own_x]
    hidden, active, slope, slot_x = forward(meta, local_x, own_x, sib_x, gate_w, up_w)
    out_twin = swap(out_half(meta, hidden, down_w, None, experts))
    out_blocks = out_half(meta, hidden, down_w, out_twin, experts)
    sib_dy = [swap(block) for block in own_dy]
    sib_dy, out_blocks = lax.optimization_barrier((sib_dy, out_blocks))
    gate_dy, up_dy, slot_dy = hidden_grads(meta, local_dy, own_dy, sib_dy, down_w, active, slope)
    back_twin = swap(back_half(meta, gate_dy, up_dy, gate_w, up_w, None, experts))
    back_blocks = back_half(meta, gate_dy, up_dy, gate_w, up_w, back_twin, experts)
    hidden, slot_x, back_blocks = lax.optimization_barrier((hidden, slot_x, back_blocks))
    grad_down = down_grad(meta, hidden, slot_dy)
    grad_gate, grad_up = in_grads(meta, slot_x, gate_dy, up_dy)
    output = reduce_tokens(out_blocks, True)
    input_grad = reduce_tokens(back_blocks, False)
    return (output, input_grad, grad_gate[None], grad_up[None], grad_down[None])


def solution(mesh):
    return jax.shard_map(
        on_device,
        mesh=mesh,
        in_specs=(
            P("dp", None),
            P("dp", None),
            P("dp", None),
            P("dp", None),
            P("dp", None, "fsdp"),
            P("dp", None, "fsdp"),
            P("dp", "fsdp", None),
        ),
        out_specs=(
            P("dp", None),
            P("dp", None),
            P("dp", None, "fsdp"),
            P("dp", None, "fsdp"),
            P("dp", "fsdp", None),
        ),
        check_vma=False,
    )
```

```python
import functools
import jax
import jax.numpy as jnp
from jax import lax
from jax.experimental import pallas as pl
from jax.experimental.pallas import tpu as pltpu
from jax.sharding import PartitionSpec as P

F32 = jnp.float32
BF16 = jnp.bfloat16
LEAD = (((0,), (0,)), ((), ()))
TRAIL = (((1,), (1,)), ((), ()))
VMEM_BYTES = 48 * 1024 * 1024


def dot(lhs, rhs, dims=None):
    if dims is None:
        return jnp.dot(lhs, rhs, preferred_element_type=F32)
    return lax.dot_general(lhs, rhs, dims, preferred_element_type=F32)


def call(body, meta, operands, in_specs, out_specs, out_shape, grid, flops, scratch=()):
    return pl.pallas_call(
        body,
        grid_spec=pltpu.PrefetchScalarGridSpec(
            num_scalar_prefetch=1,
            grid=grid,
            in_specs=in_specs,
            out_specs=out_specs,
            scratch_shapes=scratch,
        ),
        out_shape=out_shape,
        compiler_params=pltpu.CompilerParams(
            dimension_semantics=("arbitrary",) * len(grid), vmem_limit_bytes=VMEM_BYTES
        ),
        cost_estimate=pl.CostEstimate(
            flops=flops, transcendentals=0, bytes_accessed=sum(v.size * 2 for v in operands)
        ),
    )(meta, *operands)


def whole(*shape):
    return pl.BlockSpec(shape, lambda *_: (0,) * len(shape))


def array(*shape):
    return jax.ShapeDtypeStruct(shape, BF16)


def in_hbm(value):
    return pltpu.with_memory_space_constraint(value, pltpu.HBM)


def pick_tables(place_id, routes, weights, experts, capacity):
    tok_rows = routes.shape[1]
    lanes = (-(-experts // 8) * 8, tok_rows)
    ids = lax.broadcasted_iota(jnp.int32, lanes, 0) ^ place_id
    first = routes[0:1, :] == ids
    second = routes[1:2, :] == ids
    hits = jnp.where(first, 1.0, 0.0) + jnp.where(second, 1.0, 0.0)
    weight = jnp.where(first, weights[0:1, :], 0.0) + jnp.where(second, weights[1:2, :], 0.0)
    square = (tok_rows, tok_rows)
    earlier = lax.broadcasted_iota(jnp.int32, square, 0) < lax.broadcasted_iota(jnp.int32, square, 1)
    before = dot(hits.astype(BF16), jnp.where(earlier, 1.0, 0.0).astype(BF16))
    place = jnp.where(hits > 0.5, before, -1.0).astype(jnp.int32)
    slots = lax.broadcasted_iota(jnp.int32, (capacity, tok_rows), 0)
    picked = []
    weighted = []
    for expert in range(experts):
        match = place[expert : expert + 1, :] == slots
        picked.append(jnp.where(match, 1.0, 0.0))
        weighted.append(jnp.where(match, weight[expert : expert + 1, :], 0.0))
    return picked, weighted


def gather_body(meta, routes, weights, source, source_half, *outs, capacity, scaled):
    experts = len(outs)
    picked, weighted = pick_tables(meta[1], routes[...], weights[...], experts, capacity)
    for j, out in enumerate(outs):
        rows = dot(picked[j].astype(BF16), source_half[...] if j else source[...])
        if scaled:
            rows = rows * jnp.sum(weighted[j], axis=1, keepdims=True)
        out[...] = rows.astype(BF16)


def gather_rows(meta, routes, weights, source, experts, capacity, scaled):
    tok_rows, features = source.shape
    half = features // 2
    source = in_hbm(source)
    return call(
        functools.partial(gather_body, capacity=capacity, scaled=scaled),
        meta,
        (routes, weights, source, source),
        [
            whole(2, tok_rows),
            whole(2, tok_rows),
            whole(tok_rows, features),
            pl.BlockSpec((tok_rows, half), lambda i, m: (0, m[0])),
        ],
        [whole(capacity, features)] + [whole(capacity, half)] * (experts - 1),
        [array(capacity, features)] + [array(capacity, half)] * (experts - 1),
        (1,),
        2 * experts * capacity * tok_rows * half,
    )


def merge_body(meta, routes, weights, *refs, experts, capacity, scaled):
    slots = refs[:experts]
    send, keep, total = refs[experts:]
    picked, weighted = pick_tables(meta[1], routes[...], weights[...], experts, capacity)
    acc = None
    for j in range(experts):
        if scaled:
            high = weighted[j].astype(BF16)
            low = (weighted[j] - high.astype(F32)).astype(BF16)
            term = dot(high, slots[j][...], LEAD) + dot(low, slots[j][...], LEAD)
        else:
            term = dot(picked[j].astype(BF16), slots[j][...], LEAD)
        acc = term if acc is None else acc + term
    total[...] = acc
    count = send.shape[0]
    send[...] = total[pl.ds(pl.multiple_of((1 - meta[2]) * count, count), count), :].astype(BF16)
    keep[...] = total[pl.ds(pl.multiple_of(meta[2] * count, count), count), :].astype(BF16)


def merge_rows(meta, routes, weights, slots, scaled):
    experts = len(slots)
    tok_rows = routes.shape[1]
    capacity, half = slots[0].shape
    return call(
        functools.partial(merge_body, experts=experts, capacity=capacity, scaled=scaled),
        meta,
        (routes, weights, *slots),
        [whole(2, tok_rows), whole(2, tok_rows)] + [whole(capacity, half)] * experts,
        [whole(tok_rows // 2, half)] * 2,
        [array(tok_rows // 2, half)] * 2,
        (1,),
        4 * experts * capacity * tok_rows * half,
        [pltpu.VMEM((tok_rows, half), F32)],
    )


def fill_slots(meta, local, own, sib, slots):
    capacity, features = local.shape
    half = features // 2
    slots[0:capacity, :] = local[...]
    for side in range(2):

        @pl.when(meta[0] == side)
        def _():
            for j in range(len(own)):
                rows = slice((j + 1) * capacity, (j + 2) * capacity)
                mine = slice(side * half, (side + 1) * half)
                other = slice((1 - side) * half, (2 - side) * half)
                slots[rows, mine] = own[j][...]
                slots[rows, other] = sib[j][...]


def forward_body(meta, *refs, others):
    local = refs[0]
    own = refs[1 : 1 + others]
    sib = refs[1 + others : 1 + 2 * others]
    gate_w, up_w, hidden, active, slope, slots = refs[1 + 2 * others :]

    @pl.when(pl.program_id(0) == 0)
    def _():
        fill_slots(meta, local, own, sib, slots)

    gate = dot(slots[...], gate_w[...])
    up = dot(slots[...], up_w[...])
    sigma = jax.nn.sigmoid(gate)
    act = gate * sigma
    hidden[...] = (act * up).astype(BF16)
    active[...] = act.astype(BF16)
    slope[...] = (up * sigma * (1.0 + gate * (1.0 - sigma))).astype(BF16)


def forward(meta, local, own, sib, gate_w, up_w):
    capacity = local.shape[0]
    others = len(own)
    rows = capacity * (others + 1)
    features, width = gate_w.shape
    half = features // 2
    step = min(256, width)
    column = pl.BlockSpec((features, step), lambda i, m: (0, i))
    result = pl.BlockSpec((rows, step), lambda i, m: (0, i))
    return call(
        functools.partial(forward_body, others=others),
        meta,
        (local, *own, *sib, gate_w, up_w),
        [whole(capacity, features)] + [whole(capacity, half)] * (2 * others) + [column] * 2,
        [result] * 3 + [whole(rows, features)],
        [array(rows, width)] * 3 + [array(rows, features)],
        (width // step,),
        4 * rows * features * width,
    )


def out_other_body(meta, hidden, down_w, out):
    out[...] = dot(hidden[...], down_w[...]).astype(BF16)


def out_mine_body(meta, hidden, twin, down_w, *outs):
    total = dot(hidden[...], down_w[...]) + twin[...].astype(F32)
    capacity = outs[0].shape[0]
    for j, out in enumerate(outs):
        out[...] = total[j * capacity : (j + 1) * capacity, :].astype(BF16)


def out_half(meta, hidden, down_w, twin, experts):
    rows, width = hidden.shape
    half = down_w.shape[1] // 2
    step = half // 3
    tile = pl.BlockSpec((rows, step), lambda i, m: (0, i))
    if twin is None:
        return call(
            out_other_body,
            meta,
            (hidden, down_w),
            [whole(rows, width), pl.BlockSpec((width, step), lambda i, m: (0, i + 3 * (1 - m[0])))],
            tile,
            array(rows, half),
            (3,),
            2 * rows * half * width,
        )
    return call(
        out_mine_body,
        meta,
        (hidden, twin, down_w),
        [whole(rows, width), tile, pl.BlockSpec((width, step), lambda i, m: (0, i + 3 * m[0]))],
        [pl.BlockSpec((rows // experts, step), lambda i, m: (0, i))] * experts,
        [array(rows // experts, half)] * experts,
        (3,),
        2 * rows * half * width,
    )


def hidden_body(meta, *refs, others):
    local = refs[0]
    own = refs[1 : 1 + others]
    sib = refs[1 + others : 1 + 2 * others]
    down_w, active, slope, gate_dy, up_dy, slots = refs[1 + 2 * others :]

    @pl.when(pl.program_id(0) == 0)
    def _():
        fill_slots(meta, local, own, sib, slots)

    hidden_dy = dot(slots[...], down_w[...], TRAIL)
    gate_dy[...] = (hidden_dy * slope[...].astype(F32)).astype(BF16)
    up_dy[...] = (hidden_dy * active[...].astype(F32)).astype(BF16)


def hidden_grads(meta, local, own, sib, down_w, active, slope):
    capacity, features = local.shape
    others = len(own)
    rows = capacity * (others + 1)
    half = features // 2
    width = down_w.shape[0]
    step = min(256, width)
    result = pl.BlockSpec((rows, step), lambda i, m: (0, i))
    return call(
        functools.partial(hidden_body, others=others),
        meta,
        (local, *own, *sib, down_w, active, slope),
        [whole(capacity, features)]
        + [whole(capacity, half)] * (2 * others)
        + [pl.BlockSpec((step, features), lambda i, m: (i, 0)), result, result],
        [result] * 2 + [whole(rows, features)],
        [array(rows, width)] * 2 + [array(rows, features)],
        (width // step,),
        2 * rows * features * width,
    )


def back_other_body(meta, gate_dy, up_dy, gate_w, up_w, out):
    total = dot(gate_dy[...], gate_w[...], TRAIL) + dot(up_dy[...], up_w[...], TRAIL)
    out[...] = total.astype(BF16)


def back_mine_body(meta, gate_dy, up_dy, twin, gate_w, up_w, *outs):
    total = dot(gate_dy[...], gate_w[...], TRAIL) + dot(up_dy[...], up_w[...], TRAIL)
    total = total + twin[...].astype(F32)
    capacity = outs[0].shape[0]
    for j, out in enumerate(outs):
        out[...] = total[j * capacity : (j + 1) * capacity, :].astype(BF16)


def back_half(meta, gate_dy, up_dy, gate_w, up_w, twin, experts):
    rows, width = gate_dy.shape
    half = gate_w.shape[0] // 2
    step = half // 3
    tile = pl.BlockSpec((rows, step), lambda i, m: (0, i))
    if twin is None:
        block = pl.BlockSpec((step, width), lambda i, m: (i + 3 * (1 - m[0]), 0))
        return call(
            back_other_body,
            meta,
            (gate_dy, up_dy, gate_w, up_w),
            [whole(rows, width), whole(rows, width), block, block],
            tile,
            array(rows, half),
            (3,),
            4 * rows * half * width,
        )
    block = pl.BlockSpec((step, width), lambda i, m: (i + 3 * m[0], 0))
    return call(
        back_mine_body,
        meta,
        (gate_dy, up_dy, twin, gate_w, up_w),
        [whole(rows, width), whole(rows, width), tile, block, block],
        [pl.BlockSpec((rows // experts, step), lambda i, m: (0, i))] * experts,
        [array(rows // experts, half)] * experts,
        (3,),
        4 * rows * half * width,
    )


def down_grad_body(meta, hidden, slot_dy, out):
    out[...] = dot(hidden[...], slot_dy[...], LEAD).astype(BF16)


def down_grad(meta, hidden, slot_dy):
    rows, width = hidden.shape
    features = slot_dy.shape[1]
    step = features // 6
    return call(
        down_grad_body,
        meta,
        (hidden, slot_dy),
        [whole(rows, width), pl.BlockSpec((rows, step), lambda i, m: (0, i))],
        pl.BlockSpec((width, step), lambda i, m: (0, i)),
        array(width, features),
        (6,),
        2 * rows * features * width,
    )


def in_grads_body(meta, slot_x, gate_dy, up_dy, gate_out, up_out):
    gate_out[...] = dot(slot_x[...], gate_dy[...], LEAD).astype(BF16)
    up_out[...] = dot(slot_x[...], up_dy[...], LEAD).astype(BF16)


def in_grads(meta, slot_x, gate_dy, up_dy):
    rows, width = gate_dy.shape
    features = slot_x.shape[1]
    step = features // 6
    result = pl.BlockSpec((step, width), lambda i, m: (i, 0))
    return call(
        in_grads_body,
        meta,
        (slot_x, gate_dy, up_dy),
        [pl.BlockSpec((rows, step), lambda i, m: (0, i)), whole(rows, width), whole(rows, width)],
        [result, result],
        [array(features, width)] * 2,
        (6,),
        4 * rows * features * width,
    )


def assemble_body(meta, total, other, twin_total, twin_other, out):
    count, half = total.shape
    for keep in range(2):
        for side in range(2):

            @pl.when((meta[2] == keep) & (meta[0] == side))
            def _():
                held = slice(keep * count, (keep + 1) * count)
                rest = slice((1 - keep) * count, (2 - keep) * count)
                mine = slice(side * half, (side + 1) * half)
                theirs = slice((1 - side) * half, (2 - side) * half)
                out[held, mine] = total[...]
                out[rest, mine] = other[...]
                out[held, theirs] = twin_total[...]
                out[rest, theirs] = twin_other[...]


def assemble(meta, total, other, twin_total, twin_other):
    count, half = total.shape
    return call(
        assemble_body,
        meta,
        (total, other, twin_total, twin_other),
        [whole(count, half)] * 4,
        whole(2 * count, 2 * half),
        array(2 * count, 2 * half),
        (1,),
        0,
    )


def on_device(tokens, cotangent, routes, router_weight, w_gate, w_up, w_down):
    experts = lax.axis_size("dp")
    shards = lax.axis_size("fsdp")
    tok_rows, _ = tokens.shape
    capacity = max(tok_rows * 3 // 8, tok_rows * 2 // experts, 2)
    chips = shards // 2
    core = lax.axis_index("fsdp") & 1
    chip = lax.axis_index("fsdp") >> 1
    keep = (chip ^ (chip >> 1)) & 1 if chips > 2 else chip & 1
    meta = jnp.stack([core, lax.axis_index("dp"), keep]).astype(jnp.int32)
    routes_t = in_hbm(routes.T)
    weights_t = in_hbm(router_weight.T)
    gate_w = w_gate[0]
    up_w = w_up[0]
    down_w = w_down[0]

    def across(value, axis, offset, size):
        return lax.ppermute(value, axis, [(i, i ^ offset) for i in range(size)])

    def swap(value):
        return across(value, "fsdp", 1, shards)

    def hop(value, offset):
        return across(value, "fsdp", 2 * offset, shards)

    def exchange(blocks):
        return [across(block, "dp", j + 1, experts) for j, block in enumerate(blocks)]

    def reduce_tokens(blocks, scaled):
        slots = [blocks[0]] + exchange(blocks[1:])
        send, total = merge_rows(meta, routes_t, weights_t, slots, scaled)
        add = lambda a, b: (a.astype(F32) + b.astype(F32)).astype(BF16)
        moved = hop(send, 1)
        total = add(total, moved)
        offset = 2
        while offset < chips:
            moved = hop(total, 3 if offset == 2 else offset)
            total = add(total, moved)
            offset *= 2
        other = hop(total, 1)
        return assemble(meta, total, other, swap(total), swap(other))

    def step(fn, *args):
        return fn(meta, *args)

    local_x, *send_x = gather_rows(meta, routes_t, weights_t, tokens, experts, capacity, False)
    own_x = exchange(send_x)
    local_dy, *send_dy = gather_rows(meta, routes_t, weights_t, cotangent, experts, capacity, True)
    own_dy = exchange(send_dy)
    sib_x = [swap(block) for block in own_x]
    hidden, active, slope, slot_x = step(forward, local_x, own_x, sib_x, gate_w, up_w)
    out_twin = swap(step(out_half, hidden, down_w, None, experts))
    out_blocks = step(out_half, hidden, down_w, out_twin, experts)
    sib_dy = [swap(block) for block in own_dy]
    sib_dy, out_blocks = lax.optimization_barrier((sib_dy, out_blocks))
    gate_dy, up_dy, slot_dy = step(hidden_grads, local_dy, own_dy, sib_dy, down_w, active, slope)
    back_twin = swap(step(back_half, gate_dy, up_dy, gate_w, up_w, None, experts))
    back_blocks = step(back_half, gate_dy, up_dy, gate_w, up_w, back_twin, experts)
    hidden, slot_x, back_blocks = lax.optimization_barrier((hidden, slot_x, back_blocks))
    grad_down = step(down_grad, hidden, slot_dy)
    grad_gate, grad_up = step(in_grads, slot_x, gate_dy, up_dy)
    output = reduce_tokens(out_blocks, True)
    input_grad = reduce_tokens(back_blocks, False)
    return (output, input_grad, grad_gate[None], grad_up[None], grad_down[None])


def solution(mesh):
    return jax.shard_map(
        on_device,
        mesh=mesh,
        in_specs=(
            P("dp", None),
            P("dp", None),
            P("dp", None),
            P("dp", None),
            P("dp", None, "fsdp"),
            P("dp", None, "fsdp"),
            P("dp", "fsdp", None),
        ),
        out_specs=(
            P("dp", None),
            P("dp", None),
            P("dp", None, "fsdp"),
            P("dp", None, "fsdp"),
            P("dp", "fsdp", None),
        ),
        check_vma=False,
    )
```
